32 devices in a mesh: row: 4 (over y, x), col: 8 (over z, core).
Axes of the slice: x: 2, y: 2, z: 4, core: 2. Of those that a mesh axis runs over, the one named last changes fastest.
Arguments:
- depth: float32 [256, 4096], P('row', 'col'), may hold values from 0 to 1
- rainfall: float32 [256, 4096], P('row', 'col'), may hold values from 0.05 to 0.5
- conveyance: float32 [256, 4096], P('row', 'col'), may hold values from 0.2 to 5
- flow_dir: int32 [256, 4096], P('row', 'col'), may hold values from 0 to 7, as said below
- outlet: int32 [256, 4096], P('row', 'col'), may hold values 0 or 1
Outputs:
- new_depth: float32 [256, 4096], P('row', 'col')
- discharge: float32 [256, 4096], P('row', 'col')
The draws below stay inside these ranges and needn't reach their ends.
Inputs may be any that keep to these rules, and one draw needn't show every extreme that they name: `flow_dir`: each cell's code is 0 to 7.
All inputs are finite; a program needn't handle non-finite values. No bound on the sum of `outlet` on one device may be relied on, other than what follows from the above.
Results may differ from the reference program's by a relative error of at most 0.00002.
Values sent between devices are 32-bit elements; how exact they have to be, the bound alone decides.
A program may use at most 64 MiB of HBM per device.

```python
import math
import jax
import jax.numpy as jnp

SUBSTEPS = 3
PASSES = 64
NR = 256
NC = 4096


def draw_flow_dir(key, part):
    first = jax.random.fold_in(key, 11)
    second = jax.random.fold_in(key, 12)
    third = jax.random.fold_in(key, 13)
    picker = jax.random.randint(first, (NR, NC), 0, 10)
    drift = jax.random.randint(second, (NR, NC), 0, 3)
    anyway = jax.random.randint(third, (NR, NC), 0, 8)
    return jnp.where(picker < 7, drift, anyway).astype(jnp.int32)


def plant(array, key, low, top_value):
    longest = array.shape.index(max(array.shape))
    spots = []
    for shift in (0, 1):
        where = [jax.random.randint(jax.random.fold_in(key, axis), (), 0, length) for axis, length in enumerate(array.shape)]
        where[longest] = (where[longest] + shift) % array.shape[longest]
        spots.append(tuple(where))
    return array.at[spots[0]].set(low).at[spots[1]].set(top_value)


def levels(own_key, extent, split, low, largest):
    def one(axis_at, blocks):
        draws = jax.random.uniform(jax.random.fold_in(jax.random.fold_in(own_key, 6), axis_at), (blocks,), jnp.float32, low / len(split), largest / len(split))
        return jnp.repeat(jnp.exp(draws), extent[axis_at] // blocks).reshape((-1,) + (1,) * (len(extent) - axis_at - 1))

    gain = one(*split[0])
    for cut in split[1:]:
        gain = gain * one(*cut)
    return gain


def setup_inputs(seed: int = 0) -> dict:
    arg_keys = jax.random.split(jax.random.key(seed), 6)
    depth = jnp.clip(1.0 * jax.random.uniform(arg_keys[0], (NR, NC), jnp.float32) ** levels(arg_keys[0], (NR, NC), ((0, 4), (1, 8)), -0.2, 0.2), 0.0, 1.0)
    rainfall = jnp.clip(jnp.exp(math.log(0.5) - 2.3025851 * jax.random.uniform(arg_keys[1], (NR, NC), jnp.float32) ** levels(arg_keys[1], (NR, NC), ((0, 4), (1, 8)), -0.2, 0.2)), 0.05, 0.5)
    conveyance = jnp.clip(jnp.exp(math.log(5.0) - 3.218876 * jax.random.uniform(arg_keys[2], (NR, NC), jnp.float32) ** levels(arg_keys[2], (NR, NC), ((0, 4), (1, 8)), -0.2, 0.2)), 0.2, 5.0)
    flow_dir = draw_flow_dir(jax.random.fold_in(arg_keys[5], 71), 0)
    outlet = plant((jax.random.randint(arg_keys[4], (NR, NC), 0, 32) < 1).astype(jnp.int32), jax.random.fold_in(arg_keys[4], 1), 0, 1)
    return dict(depth=depth, rainfall=rainfall, conveyance=conveyance, flow_dir=flow_dir, outlet=outlet)


OFFSETS = ((0, 1), (1, 1), (1, 0), (1, -1), (0, -1), (-1, -1), (-1, 0), (-1, 1))


def inflow(sent, route):
    sent_pad = jnp.pad(sent, 1)
    route_pad = jnp.pad(route, 1)
    rows, cols = sent.shape
    total = jnp.zeros((rows, cols), jnp.float32)
    for k, (di, dj) in enumerate(OFFSETS):
        source = sent_pad[1 - di:1 - di + rows, 1 - dj:1 - dj + cols]
        target = route_pad[1 - di:1 - di + rows, 1 - dj:1 - dj + cols]
        total = total + jnp.where(target == k + 1, source, jnp.float32(0.0))
    return total


def reference(depth, rainfall, conveyance, flow_dir, outlet):
    route = jnp.where(outlet == 1, 0, flow_dir + 1).astype(jnp.int32)
    length = jnp.where(flow_dir % 2 == 1, jnp.float32(0.70710678), jnp.float32(1.0))
    level = depth
    for step in range(SUBSTEPS):
        factor = conveyance * length * jnp.power(level, jnp.float32(2.0 / 3.0))
        share = factor / (1.0 + factor)
        out = level * share
        sent = jnp.where(route > 0, out, jnp.float32(0.0))
        level = level + rainfall - out + inflow(sent, route)

    def one_pass(index, acc):
        sent = jnp.where(route > 0, acc, jnp.float32(0.0))
        return level + inflow(sent, route)

    acc = jax.lax.fori_loop(0, PASSES, one_pass, level)
    return level, jnp.log(1.0 + acc)
```

```python
import functools

import jax
import jax.numpy as jnp
from jax import lax
from jax.experimental import pallas as pl
from jax.experimental.pallas import tpu as pltpu
from jax.sharding import PartitionSpec as P

SUBSTEPS = 3
PASSES = 64
OFFSETS = ((0, 1), (1, 1), (1, 0), (1, -1), (0, -1), (-1, -1), (-1, 0), (-1, 1))
LANES = 128
SUB = 8
MARGIN = 24
GROUPS = (20, 22, 22)
MESH = pl.DeviceIdType.MESH


def kernel(
    row_peers, col_peers,
    depth_ref, rain_ref, conv_ref, dir_ref, outlet_ref,
    level_ref, discharge_ref,
    depth_ext, rain_ext, coef_ext, route_ext, acc_ext, plain,
    acc, rain, coef, level, share, masks,
    send_sem, recv_sem,
):
    rows, cols = depth_ref.shape
    total = rows + 2 * MARGIN
    bands = total // SUB
    wide = cols + LANES
    own = cols // LANES
    my_row, my_col = lax.axis_index("row"), lax.axis_index("col")

    def exists(dr, dc):
        r, c = my_row + dr, my_col + dc
        ok = None
        for test in ((r >= 0, r < row_peers) if dr else ()) + ((c >= 0, c < col_peers) if dc else ()):
            ok = test if ok is None else jnp.logical_and(ok, test)
        return ok

    def row_place(dr):
        if dr == 0:
            return (pl.ds(0, rows), pl.ds(0, rows))
        if dr < 0:
            return (pl.ds(0, MARGIN), pl.ds(rows, MARGIN))
        return (pl.ds(rows - MARGIN, MARGIN), pl.ds(rows + MARGIN, MARGIN))

    def col_place(dc):
        if dc == 0:
            return (pl.ds(0, own), pl.ds(0, own))
        if dc < 0:
            return (pl.ds(0, 1), pl.ds(own, 1))
        return (pl.ds(own - 1, 1), pl.ds(own + 1, 1))

    def copy(slot, k, src, dst):
        dr, dc = OFFSETS[k]
        (rs, rd), (cs, cd) = row_place(dr), col_place(dc)
        return pltpu.make_async_remote_copy(
            src_ref=src.at[cs, rs],
            dst_ref=dst.at[cd, rd],
            send_sem=send_sem.at[slot, k],
            recv_sem=recv_sem.at[slot, k],
            device_id=(my_row + dr, my_col + dc),
            device_id_type=MESH,
        )

    order = (1, 3, 5, 7, 2, 6, 0, 4)

    def send(slot, src, dst):
        for k in order:
            @pl.when(exists(*OFFSETS[k]))
            def _(k=k):
                copy(slot, k, src, dst).start()

    def receive(slot, src, dst):
        for k in order:
            dr, dc = OFFSETS[k]
            there = exists(-dr, -dc)

            @pl.when(there)
            def _(k=k):
                copy(slot, k, src, dst).wait_recv()

            @pl.when(jnp.logical_not(there))
            def _(dr=dr, dc=dc):
                _, rd = row_place(dr)
                _, cd = col_place(dc)
                dst[cd, rd] = jnp.zeros((cd.size, rd.size, LANES), dst.dtype)

    def sent_out(slot, src, dst):
        for k in order:
            @pl.when(exists(*OFFSETS[k]))
            def _(k=k):
                copy(slot, k, src, dst).wait_send()

    barrier = pltpu.get_barrier_semaphore()
    for dr, dc in OFFSETS:
        @pl.when(exists(dr, dc))
        def _(dr=dr, dc=dc):
            pl.semaphore_signal(
                barrier, inc=1, device_id=(my_row + dr, my_col + dc), device_id_type=MESH
            )
    for c in range(own):
        at = pl.ds(c * LANES, LANES)
        mine = pl.ds(0, rows)
        depth_ext[c, mine] = depth_ref[:, at]
        rain_ext[c, mine] = rain_ref[:, at]
        code = dir_ref[:, at]
        route_ext[c, mine] = jnp.where(outlet_ref[:, at] == 1, 0, code + 1)
        coef_ext[c, mine] = conv_ref[:, at] * jnp.where(
            (code & 1) == 1, jnp.float32(0.70710678), jnp.float32(1.0)
        )
    def reach(index, peers):
        return 1 + jnp.where(index > 0, 1, 0) + jnp.where(index < peers - 1, 1, 0)

    pl.semaphore_wait(barrier, reach(my_row, row_peers) * reach(my_col, col_peers) - 1)

    firsts = (depth_ext, coef_ext, rain_ext, route_ext)
    for slot, ext in enumerate(firsts):
        send(slot, ext, ext)
    for slot, ext in enumerate(firsts):
        receive(slot, ext, ext)

    right = lax.broadcasted_iota(jnp.int32, (SUB, LANES), 1) < LANES // 2

    def banded(ext, v):
        def part(c):
            return ext[c, pl.ds(v, SUB, stride=bands), :]

        blocks = [part(c) for c in range(own)]
        blocks.append(jnp.where(right, part(own), part(own + 1)))
        return jnp.concatenate(blocks, axis=1)

    for v in range(bands):
        acc[v] = banded(depth_ext, v)
        rain[v] = banded(rain_ext, v)
        coef[v] = banded(coef_ext, v)

    def above(v, get):
        return get(v - 1) if v else pltpu.roll(get(bands - 1), 1, 0)

    def below(v, get):
        return get(v + 1) if v < bands - 1 else pltpu.roll(get(0), SUB - 1, 0)

    def routed(v):
        return banded(route_ext, v)

    for v in range(bands):
        near = {1: above(v, routed), 0: routed(v), -1: below(v, routed)}
        for k, (di, dj) in enumerate(OFFSETS):
            masks[k, v] = jnp.where(near[di] == k + 1, jnp.float32(1.0), jnp.float32(0.0))

    def inflow(v, up, here, down):
        near = {1: up, 0: here, -1: down}
        parts = {}
        for k, (di, dj) in enumerate(OFFSETS):
            term = masks[k, v] * near[di]
            parts[dj] = parts[dj] + term if dj in parts else term
        return parts[0] + (pltpu.roll(parts[1], 1, 1) + pltpu.roll(parts[-1], wide - 1, 1))

    def sweep(field, finish):
        start = field[0]
        up, here = (pltpu.roll(field[bands - 1], 1, 0), start)
        for v in range(bands):
            down = field[v + 1] if v < bands - 1 else pltpu.roll(start, SUB - 1, 0)
            finish(v, inflow(v, up, here, down))
            up, here = here, down

    @pl.loop(0, SUBSTEPS)
    def _(step):
        for v in range(bands):
            h = acc[v]
            factor = coef[v] * jnp.exp(jnp.log(h) * jnp.float32(2.0 / 3.0))
            out = h * (factor / (1.0 + factor))
            share[v] = out
            level[v] = h + rain[v] - out

        def finish(v, came):
            acc[v] = level[v] + came

        sweep(share, finish)

    for v in range(bands):
        level[v] = acc[v]

    def finish(v, came):
        acc[v] = level[v] + came

    def passes(count):
        @pl.loop(0, count)
        def _(index):
            sweep(acc, finish)

    def to_plain(field, dst):
        for v in range(bands):
            value = field[v]
            for c in range(own):
                dst[c, pl.ds(v, SUB, stride=bands), :] = value[:, c * LANES : (c + 1) * LANES]

    passes(GROUPS[0])
    to_plain(level, plain.at[len(GROUPS) - 1])
    for c in range(own):
        level_ref[:, pl.ds(c * LANES, LANES)] = plain[len(GROUPS) - 1, c, pl.ds(0, rows), :]
    sub = lax.broadcasted_iota(jnp.int32, (SUB, LANES), 0)
    for group in range(1, len(GROUPS)):
        slot = len(firsts) + group - 1
        src, dst = plain.at[group - 1], acc_ext.at[group - 1]
        to_plain(acc, src)
        send(slot, src, dst)
        receive(slot, src, dst)
        for v in range(bands):
            inner = sub * bands + v < rows
            for c in range(own):
                at = pl.ds(c * LANES, LANES)
                acc[v, :, at] = jnp.where(
                    inner, acc[v, :, at], dst[c, pl.ds(v, SUB, stride=bands), :]
                )
            acc[v, :, pl.ds(cols, LANES)] = jnp.where(
                right,
                dst[own, pl.ds(v, SUB, stride=bands), :],
                dst[own + 1, pl.ds(v, SUB, stride=bands), :],
            )
        passes(GROUPS[group])

    to_plain(acc, plain.at[len(GROUPS)])
    for c in range(own):
        discharge_ref[:, pl.ds(c * LANES, LANES)] = jnp.log(
            1.0 + plain[len(GROUPS), c, pl.ds(0, rows), :]
        )
    for slot, ext in enumerate(firsts):
        sent_out(slot, ext, ext)
    for group in range(1, len(GROUPS)):
        sent_out(len(firsts) + group - 1, plain.at[group - 1], acc_ext.at[group - 1])


def solution(mesh):
    row_peers, col_peers = mesh.shape["row"], mesh.shape["col"]

    def on_device(depth, rainfall, conveyance, flow_dir, outlet):
        rows, cols = depth.shape
        total = rows + 2 * MARGIN
        bands = total // SUB
        wide = cols + LANES
        slots = 4 + len(GROUPS) - 1
        own = cols // LANES
        ext = (own + 2, total, LANES)
        field = (bands, SUB, wide)
        vmem = pl.BlockSpec(memory_space=pltpu.VMEM)
        f32 = jnp.float32
        return pl.pallas_call(
            functools.partial(kernel, row_peers, col_peers),
            out_shape=(jax.ShapeDtypeStruct((rows, cols), f32),) * 2,
            in_specs=[vmem] * 5,
            out_specs=(vmem, vmem),
            scratch_shapes=[
                pltpu.VMEM(ext, f32),
                pltpu.VMEM(ext, f32),
                pltpu.VMEM(ext, f32),
                pltpu.VMEM(ext, jnp.int32),
                pltpu.VMEM((len(GROUPS) - 1,) + ext, f32),
                pltpu.VMEM((len(GROUPS) + 1, own, total, LANES), f32),
                pltpu.VMEM(field, f32),
                pltpu.VMEM(field, f32),
                pltpu.VMEM(field, f32),
                pltpu.VMEM(field, f32),
                pltpu.VMEM(field, f32),
                pltpu.VMEM((len(OFFSETS),) + field, f32),
                pltpu.SemaphoreType.DMA((slots, len(OFFSETS))),
                pltpu.SemaphoreType.DMA((slots, len(OFFSETS))),
            ],
            compiler_params=pltpu.CompilerParams(collective_id=0, has_side_effects=True),
        )(depth, rainfall, conveyance, flow_dir, outlet)

    placed = P("row", "col")
    return jax.shard_map(
        on_device,
        mesh=mesh,
        in_specs=(placed,) * 5,
        out_specs=(placed, placed),
        check_vma=False,
    )
```

```python
import functools

import jax
import jax.numpy as jnp
from jax import lax
from jax.experimental import pallas as pl
from jax.experimental.pallas import tpu as pltpu
from jax.sharding import PartitionSpec as P

SUBSTEPS = 3
PASSES = 64
OFFSETS = ((0, 1), (1, 1), (1, 0), (1, -1), (0, -1), (-1, -1), (-1, 0), (-1, 1))
LANES = 128
SUB = 8
NEAR = 8
MARGIN = 32
GROUPS = PASSES // MARGIN
SPARE = 0
MESH = pl.DeviceIdType.MESH


def kernel(
    row_peers, col_peers,
    depth_ref, rain_ref, conv_ref, dir_ref, outlet_ref,
    level_ref, discharge_ref,
    depth_ext, rain_ext, coef_ext, route_ext, far_ext, acc_ext, plain,
    acc, rain, coef, level, share, masks,
    send_sem, recv_sem,
):
    rows, cols = depth_ref.shape
    total = depth_ext.shape[1]
    bands = total // SUB
    wide = cols + LANES
    own = cols // LANES
    my_row, my_col = lax.axis_index("row"), lax.axis_index("col")

    def exists(dr, dc):
        r, c = my_row + dr, my_col + dc
        ok = None
        for test in ((r >= 0, r < row_peers) if dr else ()) + ((c >= 0, c < col_peers) if dc else ()):
            ok = test if ok is None else jnp.logical_and(ok, test)
        return ok

    def row_place(dr, width):
        if dr == 0:
            return (pl.ds(0, rows), pl.ds(0, rows))
        if dr < 0:
            return (pl.ds(0, width), pl.ds(rows, width))
        return (pl.ds(rows - width, width), pl.ds(total - width, width))

    def col_place(dc):
        if dc == 0:
            return (pl.ds(0, own), pl.ds(0, own))
        if dc < 0:
            return (pl.ds(0, 1), pl.ds(own, 1))
        return (pl.ds(own - 1, 1), pl.ds(own + 1, 1))

    def copy(slot, k, src, dst, width):
        dr, dc = OFFSETS[k]
        (rs, rd), (cs, cd) = row_place(dr, width), col_place(dc)
        return pltpu.make_async_remote_copy(
            src_ref=src.at[cs, rs],
            dst_ref=dst.at[cd, rd],
            send_sem=send_sem.at[slot, k],
            recv_sem=recv_sem.at[slot, k],
            device_id=(my_row + dr, my_col + dc),
            device_id_type=MESH,
        )

    every = (1, 3, 5, 7, 2, 6, 0, 4)
    slanted = (1, 3, 5, 7, 2, 6)

    def send(slot, src, dst, width, order=every):
        for k in order:
            @pl.when(exists(*OFFSETS[k]))
            def _(k=k):
                copy(slot, k, src, dst, width).start()

    def receive(slot, src, dst, width, order=every):
        for k in order:
            dr, dc = OFFSETS[k]
            there = exists(-dr, -dc)

            @pl.when(there)
            def _(k=k):
                copy(slot, k, src, dst, width).wait_recv()

            @pl.when(jnp.logical_not(there))
            def _(dr=dr, dc=dc):
                _, rd = row_place(dr, width)
                _, cd = col_place(dc)
                dst[cd, rd] = jnp.zeros((cd.size, rd.size, LANES), dst.dtype)

    def sent_out(slot, src, dst, width, order=every):
        for k in order:
            @pl.when(exists(*OFFSETS[k]))
            def _(k=k):
                copy(slot, k, src, dst, width).wait_send()

    barrier = pltpu.get_barrier_semaphore()
    for dr, dc in OFFSETS:
        @pl.when(exists(dr, dc))
        def _(dr=dr, dc=dc):
            pl.semaphore_signal(
                barrier, inc=1, device_id=(my_row + dr, my_col + dc), device_id_type=MESH
            )
    for c in range(own):
        at = pl.ds(c * LANES, LANES)
        mine = pl.ds(0, rows)
        depth_ext[c, mine] = depth_ref[:, at]
        rain_ext[c, mine] = rain_ref[:, at]
        code = dir_ref[:, at]
        route = jnp.where(outlet_ref[:, at] == 1, 0, code + 1)
        route_ext[c, mine] = route
        far_ext[c, mine] = route
        coef_ext[c, mine] = conv_ref[:, at] * jnp.where(
            (code & 1) == 1, jnp.float32(0.70710678), jnp.float32(1.0)
        )
    def reach(index, peers):
        return 1 + jnp.where(index > 0, 1, 0) + jnp.where(index < peers - 1, 1, 0)

    pl.semaphore_wait(barrier, reach(my_row, row_peers) * reach(my_col, col_peers) - 1)

    firsts = (depth_ext, coef_ext, rain_ext, route_ext)
    far_slot, level_slot = (len(firsts), len(firsts) + 1)
    for slot, ext in enumerate(firsts):
        send(slot, ext, ext, NEAR)
    send(far_slot, far_ext, far_ext, MARGIN, slanted)
    unused = pl.ds(rows + NEAR, total - rows - 2 * NEAR)
    for ext in firsts:
        ext[:, unused] = jnp.zeros((own + 2, total - rows - 2 * NEAR, LANES), ext.dtype)
    if SPARE:
        for ext in (far_ext,) + tuple(acc_ext.at[g] for g in range(GROUPS)):
            ext[:, pl.ds(rows + MARGIN, SPARE)] = jnp.zeros((own + 2, SPARE, LANES), ext.dtype)
    for slot, ext in enumerate(firsts):
        receive(slot, ext, ext, NEAR)
    sides = (pl.ds(own, 2), pl.ds(0, rows))
    far_ext[sides] = route_ext[sides]

    right = lax.broadcasted_iota(jnp.int32, (SUB, LANES), 1) < LANES // 2

    def banded(ext, v):
        def part(c):
            return ext[c, pl.ds(v, SUB, stride=bands), :]

        blocks = [part(c) for c in range(own)]
        blocks.append(jnp.where(right, part(own), part(own + 1)))
        return jnp.concatenate(blocks, axis=1)

    for v in range(bands):
        acc[v] = banded(depth_ext, v)
        rain[v] = banded(rain_ext, v)
        coef[v] = banded(coef_ext, v)

    def above(v, get):
        return get(v - 1) if v else pltpu.roll(get(bands - 1), 1, 0)

    def below(v, get):
        return get(v + 1) if v < bands - 1 else pltpu.roll(get(0), SUB - 1, 0)

    def set_masks(ext):
        def routed(v):
            return banded(ext, v)

        for v in range(bands):
            near = {1: above(v, routed), 0: routed(v), -1: below(v, routed)}
            for k, (di, dj) in enumerate(OFFSETS):
                masks[k, v] = jnp.where(near[di] == k + 1, jnp.float32(1.0), jnp.float32(0.0))

    set_masks(route_ext)

    def inflow(v, up, here, down):
        near = {1: up, 0: here, -1: down}
        parts = {}
        for k, (di, dj) in enumerate(OFFSETS):
            term = masks[k, v] * near[di]
            parts[dj] = parts[dj] + term if dj in parts else term
        return parts[0] + (pltpu.roll(parts[1], 1, 1) + pltpu.roll(parts[-1], wide - 1, 1))

    def sweep(field, finish):
        start = field[0]
        up, here = (pltpu.roll(field[bands - 1], 1, 0), start)
        for v in range(bands):
            down = field[v + 1] if v < bands - 1 else pltpu.roll(start, SUB - 1, 0)
            finish(v, inflow(v, up, here, down))
            up, here = here, down

    @pl.loop(0, SUBSTEPS)
    def _(step):
        for v in range(bands):
            h = acc[v]
            factor = coef[v] * jnp.exp(jnp.log(h) * jnp.float32(2.0 / 3.0))
            out = h * (factor / (1.0 + factor))
            share[v] = out
            level[v] = h + rain[v] - out

        def finish(v, came):
            acc[v] = level[v] + came

        sweep(share, finish)

    def finish(v, came):
        acc[v] = level[v] + came

    def passes(count):
        @pl.loop(0, count)
        def _(index):
            sweep(acc, finish)

    def to_plain(field, dst):
        for v in range(bands):
            value = field[v]
            for c in range(own):
                dst[c, pl.ds(v, SUB, stride=bands), :] = value[:, c * LANES : (c + 1) * LANES]

    sub = lax.broadcasted_iota(jnp.int32, (SUB, LANES), 0)

    def widen(src, dst, slot, meanwhile, fields):
        to_plain(acc, src)
        send(slot, src, dst, MARGIN)
        meanwhile()
        receive(slot, src, dst, MARGIN)
        for v in range(bands):
            inner = sub * bands + v < rows
            for c in range(own):
                at = pl.ds(c * LANES, LANES)
                value = jnp.where(inner, acc[v, :, at], dst[c, pl.ds(v, SUB, stride=bands), :])
                for field in fields:
                    field[v, :, at] = value
            value = jnp.where(
                right,
                dst[own, pl.ds(v, SUB, stride=bands), :],
                dst[own + 1, pl.ds(v, SUB, stride=bands), :],
            )
            for field in fields:
                field[v, :, pl.ds(cols, LANES)] = value

    def in_flight():
        for c in range(own):
            level_ref[:, pl.ds(c * LANES, LANES)] = plain[0, c, pl.ds(0, rows), :]
        receive(far_slot, far_ext, far_ext, MARGIN, slanted)
        set_masks(far_ext)

    widen(plain.at[0], acc_ext.at[0], level_slot, in_flight, (acc, level))
    passes(MARGIN)
    for group in range(1, GROUPS):
        widen(plain.at[group], acc_ext.at[group], level_slot + group, lambda: None, (acc,))
        passes(MARGIN)

    to_plain(acc, plain.at[GROUPS])
    for c in range(own):
        discharge_ref[:, pl.ds(c * LANES, LANES)] = jnp.log(1.0 + plain[GROUPS, c, pl.ds(0, rows), :])
    for slot, ext in enumerate(firsts):
        sent_out(slot, ext, ext, NEAR)
    sent_out(far_slot, far_ext, far_ext, MARGIN, slanted)
    for group in range(GROUPS):
        sent_out(level_slot + group, plain.at[group], acc_ext.at[group], MARGIN)


def solution(mesh):
    row_peers, col_peers = mesh.shape["row"], mesh.shape["col"]

    def on_device(depth, rainfall, conveyance, flow_dir, outlet):
        rows, cols = depth.shape
        total = rows + 2 * MARGIN + SPARE
        bands = total // SUB
        wide = cols + LANES
        slots = 5 + GROUPS
        own = cols // LANES
        ext = (own + 2, total, LANES)
        field = (bands, SUB, wide)
        vmem = pl.BlockSpec(memory_space=pltpu.VMEM)
        f32 = jnp.float32
        return pl.pallas_call(
            functools.partial(kernel, row_peers, col_peers),
            out_shape=(jax.ShapeDtypeStruct((rows, cols), f32),) * 2,
            in_specs=[vmem] * 5,
            out_specs=(vmem, vmem),
            scratch_shapes=[
                pltpu.VMEM(ext, f32),
                pltpu.VMEM(ext, f32),
                pltpu.VMEM(ext, f32),
                pltpu.VMEM(ext, jnp.int32),
                pltpu.VMEM(ext, jnp.int32),
                pltpu.VMEM((GROUPS,) + ext, f32),
                pltpu.VMEM((GROUPS + 1, own, total, LANES), f32),
                pltpu.VMEM(field, f32),
                pltpu.VMEM(field, f32),
                pltpu.VMEM(field, f32),
                pltpu.VMEM(field, f32),
                pltpu.VMEM(field, f32),
                pltpu.VMEM((len(OFFSETS),) + field, f32),
                pltpu.SemaphoreType.DMA((slots, len(OFFSETS))),
                pltpu.SemaphoreType.DMA((slots, len(OFFSETS))),
            ],
            compiler_params=pltpu.CompilerParams(collective_id=0, has_side_effects=True),
        )(depth, rainfall, conveyance, flow_dir, outlet)

    placed = P("row", "col")
    return jax.shard_map(
        on_device,
        mesh=mesh,
        in_specs=(placed,) * 5,
        out_specs=(placed, placed),
        check_vma=False,
    )
```

```python
import functools

import jax
import jax.numpy as jnp
from jax import lax
from jax.experimental import pallas as pl
from jax.experimental.pallas import tpu as pltpu
from jax.sharding import PartitionSpec as P

SUBSTEPS = 3
PASSES = 64
OFFSETS = ((0, 1), (1, 1), (1, 0), (1, -1), (0, -1), (-1, -1), (-1, 0), (-1, 1))
LANES = 128
SUB = 8
NEAR = 8
MARGIN = 32
GROUPS = PASSES // MARGIN
SPARE = 0
MESH = pl.DeviceIdType.MESH


def kernel(
    row_peers, col_peers,
    depth_ref, rain_ref, conv_ref, dir_ref, outlet_ref,
    level_ref, discharge_ref,
    depth_ext, rain_ext, coef_ext, route_ext, far_ext, acc_ext, plain, pack_out, pack_in,
    acc, rain, coef, level, share, masks,
    send_sem, recv_sem,
):
    rows, cols = depth_ref.shape
    total = depth_ext.shape[1]
    bands = total // SUB
    wide = cols + LANES
    own = cols // LANES
    my_row, my_col = lax.axis_index("row"), lax.axis_index("col")

    def exists(dr, dc):
        r, c = my_row + dr, my_col + dc
        ok = None
        for test in ((r >= 0, r < row_peers) if dr else ()) + ((c >= 0, c < col_peers) if dc else ()):
            ok = test if ok is None else jnp.logical_and(ok, test)
        return ok

    def row_place(dr, width):
        if dr == 0:
            return (pl.ds(0, rows), pl.ds(0, rows))
        if dr < 0:
            return (pl.ds(0, width), pl.ds(rows, width))
        return (pl.ds(rows - width, width), pl.ds(total - width, width))

    def col_place(dc):
        if dc == 0:
            return (pl.ds(0, own), pl.ds(0, own))
        if dc < 0:
            return (pl.ds(0, 1), pl.ds(own, 1))
        return (pl.ds(own - 1, 1), pl.ds(own + 1, 1))

    def copy(slot, k, src, dst, width):
        dr, dc = OFFSETS[k]
        (rs, rd), (cs, cd) = row_place(dr, width), col_place(dc)
        return pltpu.make_async_remote_copy(
            src_ref=src.at[cs, rs],
            dst_ref=dst.at[cd, rd],
            send_sem=send_sem.at[slot, k],
            recv_sem=recv_sem.at[slot, k],
            device_id=(my_row + dr, my_col + dc),
            device_id_type=MESH,
        )

    every = (1, 3, 5, 7, 2, 6, 0, 4)
    slanted = (1, 3, 5, 7, 2, 6)
    straight, corners = (2, 6, 0, 4), (1, 3, 5, 7)

    def send(slot, src, dst, width, order=every):
        for k in order:
            @pl.when(exists(*OFFSETS[k]))
            def _(k=k):
                copy(slot, k, src, dst, width).start()

    def receive(slot, src, dst, width, order=every):
        for k in order:
            dr, dc = OFFSETS[k]
            there = exists(-dr, -dc)

            @pl.when(there)
            def _(k=k):
                copy(slot, k, src, dst, width).wait_recv()

            @pl.when(jnp.logical_not(there))
            def _(dr=dr, dc=dc):
                _, rd = row_place(dr, width)
                _, cd = col_place(dc)
                dst[cd, rd] = jnp.zeros((cd.size, rd.size, LANES), dst.dtype)

    def sent_out(slot, src, dst, width, order=every):
        for k in order:
            @pl.when(exists(*OFFSETS[k]))
            def _(k=k):
                copy(slot, k, src, dst, width).wait_send()

    barrier = pltpu.get_barrier_semaphore()
    for dr, dc in OFFSETS:
        @pl.when(exists(dr, dc))
        def _(dr=dr, dc=dc):
            pl.semaphore_signal(
                barrier, inc=1, device_id=(my_row + dr, my_col + dc), device_id_type=MESH
            )
    for c in range(own):
        at = pl.ds(c * LANES, LANES)
        mine = pl.ds(0, rows)
        depth_ext[c, mine] = depth_ref[:, at]
        rain_ext[c, mine] = rain_ref[:, at]
        code = dir_ref[:, at]
        route = jnp.where(outlet_ref[:, at] == 1, 0, code + 1)
        route_ext[c, mine] = route
        far_ext[c, mine] = route
        coef_ext[c, mine] = conv_ref[:, at] * jnp.where(
            (code & 1) == 1, jnp.float32(0.70710678), jnp.float32(1.0)
        )
    def reach(index, peers):
        return 1 + jnp.where(index > 0, 1, 0) + jnp.where(index < peers - 1, 1, 0)

    pl.semaphore_wait(barrier, reach(my_row, row_peers) * reach(my_col, col_peers) - 1)

    firsts = (depth_ext, coef_ext, rain_ext, route_ext)
    far_slot, level_slot = (len(firsts), len(firsts) + 1)
    for slot, ext in enumerate(firsts):
        send(slot, ext, ext, NEAR)
    send(far_slot, far_ext, far_ext, MARGIN, slanted)
    unused = pl.ds(rows + NEAR, total - rows - 2 * NEAR)
    for ext in firsts:
        ext[:, unused] = jnp.zeros((own + 2, total - rows - 2 * NEAR, LANES), ext.dtype)
    if SPARE:
        for ext in (far_ext,) + tuple(acc_ext.at[g] for g in range(GROUPS)):
            ext[:, pl.ds(rows + MARGIN, SPARE)] = jnp.zeros((own + 2, SPARE, LANES), ext.dtype)
    for slot, ext in enumerate(firsts):
        receive(slot, ext, ext, NEAR)
    sides = (pl.ds(own, 2), pl.ds(0, rows))
    far_ext[sides] = route_ext[sides]

    right = lax.broadcasted_iota(jnp.int32, (SUB, LANES), 1) < LANES // 2

    def banded(ext, v):
        def part(c):
            return ext[c, pl.ds(v, SUB, stride=bands), :]

        blocks = [part(c) for c in range(own)]
        blocks.append(jnp.where(right, part(own), part(own + 1)))
        return jnp.concatenate(blocks, axis=1)

    for v in range(bands):
        acc[v] = banded(depth_ext, v)
        rain[v] = banded(rain_ext, v)
        coef[v] = banded(coef_ext, v)

    def above(v, get):
        return get(v - 1) if v else pltpu.roll(get(bands - 1), 1, 0)

    def below(v, get):
        return get(v + 1) if v < bands - 1 else pltpu.roll(get(0), SUB - 1, 0)

    def set_masks(ext):
        def routed(v):
            return banded(ext, v)

        for v in range(bands):
            near = {1: above(v, routed), 0: routed(v), -1: below(v, routed)}
            for k, (di, dj) in enumerate(OFFSETS):
                masks[k, v] = jnp.where(near[di] == k + 1, jnp.float32(1.0), jnp.float32(0.0))

    set_masks(route_ext)

    def inflow(v, up, here, down):
        near = {1: up, 0: here, -1: down}
        parts = {}
        for k, (di, dj) in enumerate(OFFSETS):
            term = masks[k, v] * near[di]
            parts[dj] = parts[dj] + term if dj in parts else term
        return parts[0] + (pltpu.roll(parts[1], 1, 1) + pltpu.roll(parts[-1], wide - 1, 1))

    def sweep(field, finish):
        start = field[0]
        up, here = (pltpu.roll(field[bands - 1], 1, 0), start)
        for v in range(bands):
            down = field[v + 1] if v < bands - 1 else pltpu.roll(start, SUB - 1, 0)
            finish(v, inflow(v, up, here, down))
            up, here = here, down

    @pl.loop(0, SUBSTEPS)
    def _(step):
        for v in range(bands):
            h = acc[v]
            factor = coef[v] * jnp.exp(jnp.log(h) * jnp.float32(2.0 / 3.0))
            out = h * (factor / (1.0 + factor))
            share[v] = out
            level[v] = h + rain[v] - out

        def finish(v, came):
            acc[v] = level[v] + came

        sweep(share, finish)

    def finish(v, came):
        acc[v] = level[v] + came

    def passes(count):
        @pl.loop(0, count)
        def _(index):
            sweep(acc, finish)

    def to_plain(field, dst):
        for v in range(bands):
            value = field[v]
            for c in range(own):
                dst[c, pl.ds(v, SUB, stride=bands), :] = value[:, c * LANES : (c + 1) * LANES]

    sub = lax.broadcasted_iota(jnp.int32, (SUB, LANES), 0)

    lane_part = lax.broadcasted_iota(jnp.int32, (SUB, LANES), 1) // MARGIN

    def corner(group, k):
        dr, dc = OFFSETS[k]
        slot = level_slot + group
        return pltpu.make_async_remote_copy(
            src_ref=pack_out.at[group, k],
            dst_ref=pack_in.at[group, k],
            send_sem=send_sem.at[slot, k],
            recv_sem=recv_sem.at[slot, k],
            device_id=(my_row + dr, my_col + dc),
            device_id_type=MESH,
        )

    def send_corners(group, src):
        for k in corners:
            dr, dc = OFFSETS[k]
            start = 0 if dr < 0 else rows - MARGIN
            block, first = (0, 0) if dc < 0 else (own - 1, LANES - MARGIN)
            packed = None
            for g in range(MARGIN // SUB):
                piece = src[block, pl.ds(start + g * SUB, SUB), :]
                shift = (g * MARGIN - first) % LANES
                piece = pltpu.roll(piece, shift, 1) if shift else piece
                packed = piece if packed is None else jnp.where(lane_part == g, piece, packed)
            pack_out[group, k] = packed
        for k in corners:
            @pl.when(exists(*OFFSETS[k]))
            def _(k=k):
                corner(group, k).start()

    def receive_corners(group, dst):
        for k in corners:
            dr, dc = OFFSETS[k]
            there = exists(-dr, -dc)
            start = rows if dr < 0 else total - MARGIN
            block, first = (own, 0) if dc < 0 else (own + 1, LANES - MARGIN)

            @pl.when(there)
            def _(k=k, start=start, block=block, first=first):
                corner(group, k).wait_recv()
                packed = pack_in[group, k]
                for g in range(MARGIN // SUB):
                    shift = (first - g * MARGIN) % LANES
                    piece = pltpu.roll(packed, shift, 1) if shift else packed
                    dst[block, pl.ds(start + g * SUB, SUB), :] = piece

            @pl.when(jnp.logical_not(there))
            def _(start=start, block=block):
                dst[block, pl.ds(start, MARGIN), :] = jnp.zeros((MARGIN, LANES), dst.dtype)

    def widen(src, dst, group, meanwhile, fields):
        slot = level_slot + group
        to_plain(acc, src)
        send_corners(group, src)
        send(slot, src, dst, MARGIN, straight)
        meanwhile()
        receive(slot, src, dst, MARGIN, straight)
        receive_corners(group, dst)
        for v in range(bands):
            inner = sub * bands + v < rows
            for c in range(own):
                at = pl.ds(c * LANES, LANES)
                value = jnp.where(inner, acc[v, :, at], dst[c, pl.ds(v, SUB, stride=bands), :])
                for field in fields:
                    field[v, :, at] = value
            value = jnp.where(
                right,
                dst[own, pl.ds(v, SUB, stride=bands), :],
                dst[own + 1, pl.ds(v, SUB, stride=bands), :],
            )
            for field in fields:
                field[v, :, pl.ds(cols, LANES)] = value

    def in_flight():
        for c in range(own):
            level_ref[:, pl.ds(c * LANES, LANES)] = plain[0, c, pl.ds(0, rows), :]
        receive(far_slot, far_ext, far_ext, MARGIN, slanted)
        set_masks(far_ext)

    widen(plain.at[0], acc_ext.at[0], 0, in_flight, (acc, level))
    passes(MARGIN)
    for group in range(1, GROUPS):
        widen(plain.at[group], acc_ext.at[group], group, lambda: None, (acc,))
        passes(MARGIN)

    to_plain(acc, plain.at[GROUPS])
    for c in range(own):
        discharge_ref[:, pl.ds(c * LANES, LANES)] = jnp.log(1.0 + plain[GROUPS, c, pl.ds(0, rows), :])
    for slot, ext in enumerate(firsts):
        sent_out(slot, ext, ext, NEAR)
    sent_out(far_slot, far_ext, far_ext, MARGIN, slanted)
    for group in range(GROUPS):
        sent_out(level_slot + group, plain.at[group], acc_ext.at[group], MARGIN, straight)
        for k in corners:
            @pl.when(exists(*OFFSETS[k]))
            def _(group=group, k=k):
                corner(group, k).wait_send()


def solution(mesh):
    row_peers, col_peers = mesh.shape["row"], mesh.shape["col"]

    def on_device(depth, rainfall, conveyance, flow_dir, outlet):
        rows, cols = depth.shape
        total = rows + 2 * MARGIN + SPARE
        bands = total // SUB
        wide = cols + LANES
        slots = 5 + GROUPS
        own = cols // LANES
        ext = (own + 2, total, LANES)
        field = (bands, SUB, wide)
        vmem = pl.BlockSpec(memory_space=pltpu.VMEM)
        f32 = jnp.float32
        return pl.pallas_call(
            functools.partial(kernel, row_peers, col_peers),
            out_shape=(jax.ShapeDtypeStruct((rows, cols), f32),) * 2,
            in_specs=[vmem] * 5,
            out_specs=(vmem, vmem),
            scratch_shapes=[
                pltpu.VMEM(ext, f32),
                pltpu.VMEM(ext, f32),
                pltpu.VMEM(ext, f32),
                pltpu.VMEM(ext, jnp.int32),
                pltpu.VMEM(ext, jnp.int32),
                pltpu.VMEM((GROUPS,) + ext, f32),
                pltpu.VMEM((GROUPS + 1, own, total, LANES), f32),
                pltpu.VMEM((GROUPS, len(OFFSETS), SUB, LANES), f32),
                pltpu.VMEM((GROUPS, len(OFFSETS), SUB, LANES), f32),
                pltpu.VMEM(field, f32),
                pltpu.VMEM(field, f32),
                pltpu.VMEM(field, f32),
                pltpu.VMEM(field, f32),
                pltpu.VMEM(field, f32),
                pltpu.VMEM((len(OFFSETS),) + field, f32),
                pltpu.SemaphoreType.DMA((slots, len(OFFSETS))),
                pltpu.SemaphoreType.DMA((slots, len(OFFSETS))),
            ],
            compiler_params=pltpu.CompilerParams(collective_id=0, has_side_effects=True),
        )(depth, rainfall, conveyance, flow_dir, outlet)

    placed = P("row", "col")
    return jax.shard_map(
        on_device,
        mesh=mesh,
        in_specs=(placed,) * 5,
        out_specs=(placed, placed),
        check_vma=False,
    )
```

```python
import functools

import jax
import jax.numpy as jnp
from jax import lax
from jax.experimental import pallas as pl
from jax.experimental.pallas import tpu as pltpu
from jax.sharding import PartitionSpec as P

SUBSTEPS = 3
PASSES = 64
OFFSETS = ((0, 1), (1, 1), (1, 0), (1, -1), (0, -1), (-1, -1), (-1, 0), (-1, 1))
LANES = 128
SUB = 8
NEAR = 8
MARGIN = 32
GROUPS = PASSES // MARGIN
SPARE = 8
MESH = pl.DeviceIdType.MESH


def kernel(
    row_peers, col_peers,
    depth_ref, rain_ref, conv_ref, dir_ref, outlet_ref,
    level_ref, discharge_ref,
    depth_ext, rain_ext, coef_ext, route_ext, far_ext, acc_ext, plain, pack_out, pack_in,
    acc, rain, coef, level, share, masks,
    send_sem, recv_sem,
):
    rows, cols = depth_ref.shape
    total = depth_ext.shape[1]
    bands = total // SUB
    wide = cols + LANES
    own = cols // LANES
    my_row, my_col = lax.axis_index("row"), lax.axis_index("col")

    def exists(dr, dc):
        r, c = my_row + dr, my_col + dc
        ok = None
        for test in ((r >= 0, r < row_peers) if dr else ()) + ((c >= 0, c < col_peers) if dc else ()):
            ok = test if ok is None else jnp.logical_and(ok, test)
        return ok

    def row_place(dr, width):
        if dr == 0:
            return (pl.ds(0, rows), pl.ds(0, rows))
        if dr < 0:
            return (pl.ds(0, width), pl.ds(rows, width))
        return (pl.ds(rows - width, width), pl.ds(total - width, width))

    def col_place(dc):
        if dc == 0:
            return (pl.ds(0, own), pl.ds(0, own))
        if dc < 0:
            return (pl.ds(0, 1), pl.ds(own, 1))
        return (pl.ds(own - 1, 1), pl.ds(own + 1, 1))

    def copy(slot, k, src, dst, width):
        dr, dc = OFFSETS[k]
        (rs, rd), (cs, cd) = row_place(dr, width), col_place(dc)
        return pltpu.make_async_remote_copy(
            src_ref=src.at[cs, rs],
            dst_ref=dst.at[cd, rd],
            send_sem=send_sem.at[slot, k],
            recv_sem=recv_sem.at[slot, k],
            device_id=(my_row + dr, my_col + dc),
            device_id_type=MESH,
        )

    every = (1, 3, 5, 7, 2, 6, 0, 4)
    slanted = (1, 3, 5, 7, 2, 6)
    straight, corners = (2, 6, 0, 4), (1, 3, 5, 7)

    def send(slot, src, dst, width, order=every):
        for k in order:
            @pl.when(exists(*OFFSETS[k]))
            def _(k=k):
                copy(slot, k, src, dst, width).start()

    def receive(slot, src, dst, width, order=every):
        for k in order:
            dr, dc = OFFSETS[k]
            there = exists(-dr, -dc)

            @pl.when(there)
            def _(k=k):
                copy(slot, k, src, dst, width).wait_recv()

            @pl.when(jnp.logical_not(there))
            def _(dr=dr, dc=dc):
                _, rd = row_place(dr, width)
                _, cd = col_place(dc)
                dst[cd, rd] = jnp.zeros((cd.size, rd.size, LANES), dst.dtype)

    def sent_out(slot, src, dst, width, order=every):
        for k in order:
            @pl.when(exists(*OFFSETS[k]))
            def _(k=k):
                copy(slot, k, src, dst, width).wait_send()

    barrier = pltpu.get_barrier_semaphore()
    for dr, dc in OFFSETS:
        @pl.when(exists(dr, dc))
        def _(dr=dr, dc=dc):
            pl.semaphore_signal(
                barrier, inc=1, device_id=(my_row + dr, my_col + dc), device_id_type=MESH
            )
    for c in range(own):
        at = pl.ds(c * LANES, LANES)
        mine = pl.ds(0, rows)
        depth_ext[c, mine] = depth_ref[:, at]
        rain_ext[c, mine] = rain_ref[:, at]
        code = dir_ref[:, at]
        route = jnp.where(outlet_ref[:, at] == 1, 0, code + 1)
        route_ext[c, mine] = route
        far_ext[c, mine] = route
        coef_ext[c, mine] = conv_ref[:, at] * jnp.where(
            (code & 1) == 1, jnp.float32(0.70710678), jnp.float32(1.0)
        )
    def reach(index, peers):
        return 1 + jnp.where(index > 0, 1, 0) + jnp.where(index < peers - 1, 1, 0)

    pl.semaphore_wait(barrier, reach(my_row, row_peers) * reach(my_col, col_peers) - 1)

    firsts = (depth_ext, coef_ext, rain_ext, route_ext)
    far_slot, level_slot = (len(firsts), len(firsts) + 1)
    for slot, ext in enumerate(firsts):
        send(slot, ext, ext, NEAR)
    send(far_slot, far_ext, far_ext, MARGIN, slanted)
    unused = pl.ds(rows + NEAR, total - rows - 2 * NEAR)
    for ext in firsts:
        ext[:, unused] = jnp.zeros((own + 2, total - rows - 2 * NEAR, LANES), ext.dtype)
    if SPARE:
        for ext in (far_ext,) + tuple(acc_ext.at[g] for g in range(GROUPS)):
            ext[:, pl.ds(rows + MARGIN, SPARE)] = jnp.zeros((own + 2, SPARE, LANES), ext.dtype)
    for slot, ext in enumerate(firsts):
        receive(slot, ext, ext, NEAR)
    sides = (pl.ds(own, 2), pl.ds(0, rows))
    far_ext[sides] = route_ext[sides]

    right = lax.broadcasted_iota(jnp.int32, (SUB, LANES), 1) < LANES // 2

    def banded(ext, v):
        def part(c):
            return ext[c, pl.ds(v, SUB, stride=bands), :]

        blocks = [part(c) for c in range(own)]
        blocks.append(jnp.where(right, part(own), part(own + 1)))
        return jnp.concatenate(blocks, axis=1)

    for v in range(bands):
        acc[v] = banded(depth_ext, v)
        rain[v] = banded(rain_ext, v)
        coef[v] = banded(coef_ext, v)

    def above(v, get):
        return get(v - 1) if v else pltpu.roll(get(bands - 1), 1, 0)

    def below(v, get):
        return get(v + 1) if v < bands - 1 else pltpu.roll(get(0), SUB - 1, 0)

    def set_masks(ext):
        def routed(v):
            return banded(ext, v)

        for v in range(bands):
            near = {1: above(v, routed), 0: routed(v), -1: below(v, routed)}
            for k, (di, dj) in enumerate(OFFSETS):
                masks[k, v] = jnp.where(near[di] == k + 1, jnp.float32(1.0), jnp.float32(0.0))

    set_masks(route_ext)

    def inflow(v, up, here, down):
        near = {1: up, 0: here, -1: down}
        parts = {}
        for k, (di, dj) in enumerate(OFFSETS):
            term = masks[k, v] * near[di]
            parts[dj] = parts[dj] + term if dj in parts else term
        return parts[0] + (pltpu.roll(parts[1], 1, 1) + pltpu.roll(parts[-1], wide - 1, 1))

    def sweep(field, finish):
        start = field[0]
        up, here = (pltpu.roll(field[bands - 1], 1, 0), start)
        for v in range(bands):
            down = field[v + 1] if v < bands - 1 else pltpu.roll(start, SUB - 1, 0)
            finish(v, inflow(v, up, here, down))
            up, here = here, down

    @pl.loop(0, SUBSTEPS)
    def _(step):
        for v in range(bands):
            h = acc[v]
            factor = coef[v] * jnp.exp(jnp.log(h) * jnp.float32(2.0 / 3.0))
            out = h * (factor / (1.0 + factor))
            share[v] = out
            level[v] = h + rain[v] - out

        def finish(v, came):
            acc[v] = level[v] + came

        sweep(share, finish)

    def finish(v, came):
        acc[v] = level[v] + came

    def passes(count):
        @pl.loop(0, count)
        def _(index):
            sweep(acc, finish)

    def to_plain(field, dst):
        for v in range(bands):
            value = field[v]
            for c in range(own):
                dst[c, pl.ds(v, SUB, stride=bands), :] = value[:, c * LANES : (c + 1) * LANES]

    sub = lax.broadcasted_iota(jnp.int32, (SUB, LANES), 0)

    lane_part = lax.broadcasted_iota(jnp.int32, (SUB, LANES), 1) // MARGIN

    def corner(group, k):
        dr, dc = OFFSETS[k]
        slot = level_slot + group
        return pltpu.make_async_remote_copy(
            src_ref=pack_out.at[group, k],
            dst_ref=pack_in.at[group, k],
            send_sem=send_sem.at[slot, k],
            recv_sem=recv_sem.at[slot, k],
            device_id=(my_row + dr, my_col + dc),
            device_id_type=MESH,
        )

    def send_corners(group, src):
        for k in corners:
            dr, dc = OFFSETS[k]
            start = 0 if dr < 0 else rows - MARGIN
            block, first = (0, 0) if dc < 0 else (own - 1, LANES - MARGIN)
            packed = None
            for g in range(MARGIN // SUB):
                piece = src[block, pl.ds(start + g * SUB, SUB), :]
                shift = (g * MARGIN - first) % LANES
                piece = pltpu.roll(piece, shift, 1) if shift else piece
                packed = piece if packed is None else jnp.where(lane_part == g, piece, packed)
            pack_out[group, k] = packed
        for k in corners:
            @pl.when(exists(*OFFSETS[k]))
            def _(k=k):
                corner(group, k).start()

    def receive_corners(group, dst):
        for k in corners:
            dr, dc = OFFSETS[k]
            there = exists(-dr, -dc)
            start = rows if dr < 0 else total - MARGIN
            block, first = (own, 0) if dc < 0 else (own + 1, LANES - MARGIN)

            @pl.when(there)
            def _(k=k, start=start, block=block, first=first):
                corner(group, k).wait_recv()
                packed = pack_in[group, k]
                for g in range(MARGIN // SUB):
                    shift = (first - g * MARGIN) % LANES
                    piece = pltpu.roll(packed, shift, 1) if shift else packed
                    dst[block, pl.ds(start + g * SUB, SUB), :] = piece

            @pl.when(jnp.logical_not(there))
            def _(start=start, block=block):
                dst[block, pl.ds(start, MARGIN), :] = jnp.zeros((MARGIN, LANES), dst.dtype)

    def widen(src, dst, group, meanwhile, fields):
        slot = level_slot + group
        to_plain(acc, src)
        send_corners(group, src)
        send(slot, src, dst, MARGIN, straight)
        meanwhile()
        receive(slot, src, dst, MARGIN, straight)
        receive_corners(group, dst)
        for v in range(bands):
            inner = sub * bands + v < rows
            for c in range(own):
                at = pl.ds(c * LANES, LANES)
                value = jnp.where(inner, acc[v, :, at], dst[c, pl.ds(v, SUB, stride=bands), :])
                for field in fields:
                    field[v, :, at] = value
            value = jnp.where(
                right,
                dst[own, pl.ds(v, SUB, stride=bands), :],
                dst[own + 1, pl.ds(v, SUB, stride=bands), :],
            )
            for field in fields:
                field[v, :, pl.ds(cols, LANES)] = value

    def in_flight():
        for c in range(own):
            level_ref[:, pl.ds(c * LANES, LANES)] = plain[0, c, pl.ds(0, rows), :]
        receive(far_slot, far_ext, far_ext, MARGIN, slanted)
        set_masks(far_ext)

    widen(plain.at[0], acc_ext.at[0], 0, in_flight, (acc, level))
    passes(MARGIN)
    for group in range(1, GROUPS):
        widen(plain.at[group], acc_ext.at[group], group, lambda: None, (acc,))
        passes(MARGIN)

    to_plain(acc, plain.at[GROUPS])
    for c in range(own):
        discharge_ref[:, pl.ds(c * LANES, LANES)] = jnp.log(1.0 + plain[GROUPS, c, pl.ds(0, rows), :])
    for slot, ext in enumerate(firsts):
        sent_out(slot, ext, ext, NEAR)
    sent_out(far_slot, far_ext, far_ext, MARGIN, slanted)
    for group in range(GROUPS):
        sent_out(level_slot + group, plain.at[group], acc_ext.at[group], MARGIN, straight)
        for k in corners:
            @pl.when(exists(*OFFSETS[k]))
            def _(group=group, k=k):
                corner(group, k).wait_send()


def solution(mesh):
    row_peers, col_peers = mesh.shape["row"], mesh.shape["col"]

    def on_device(depth, rainfall, conveyance, flow_dir, outlet):
        rows, cols = depth.shape
        total = rows + 2 * MARGIN + SPARE
        bands = total // SUB
        wide = cols + LANES
        slots = 5 + GROUPS
        own = cols // LANES
        ext = (own + 2, total, LANES)
        field = (bands, SUB, wide)
        vmem = pl.BlockSpec(memory_space=pltpu.VMEM)
        f32 = jnp.float32
        return pl.pallas_call(
            functools.partial(kernel, row_peers, col_peers),
            out_shape=(jax.ShapeDtypeStruct((rows, cols), f32),) * 2,
            in_specs=[vmem] * 5,
            out_specs=(vmem, vmem),
            scratch_shapes=[
                pltpu.VMEM(ext, f32),
                pltpu.VMEM(ext, f32),
                pltpu.VMEM(ext, f32),
                pltpu.VMEM(ext, jnp.int32),
                pltpu.VMEM(ext, jnp.int32),
                pltpu.VMEM((GROUPS,) + ext, f32),
                pltpu.VMEM((GROUPS + 1, own, total, LANES), f32),
                pltpu.VMEM((GROUPS, len(OFFSETS), SUB, LANES), f32),
                pltpu.VMEM((GROUPS, len(OFFSETS), SUB, LANES), f32),
                pltpu.VMEM(field, f32),
                pltpu.VMEM(field, f32),
                pltpu.VMEM(field, f32),
                pltpu.VMEM(field, f32),
                pltpu.VMEM(field, f32),
                pltpu.VMEM((len(OFFSETS),) + field, f32),
                pltpu.SemaphoreType.DMA((slots, len(OFFSETS))),
                pltpu.SemaphoreType.DMA((slots, len(OFFSETS))),
            ],
            compiler_params=pltpu.CompilerParams(collective_id=0, has_side_effects=True),
        )(depth, rainfall, conveyance, flow_dir, outlet)

    placed = P("row", "col")
    return jax.shard_map(
        on_device,
        mesh=mesh,
        in_specs=(placed,) * 5,
        out_specs=(placed, placed),
        check_vma=False,
    )
```
